32 devices in a mesh: tx: 8 (over z, y), ty: 2 (over x), mem: 2 (over core).
Axes of the slice: x: 2, y: 2, z: 4, core: 2. Of those that a mesh axis runs over, the one named last changes fastest.
Arguments:
- obs_value: float32 [262144], P(('tx', 'ty', 'mem')), may hold values from -6 to 6
- obs_frac: float32 [2, 262144], P(None, ('tx', 'ty', 'mem')), may hold values from 0 to 1
- obs_cell: int32 [262144], P(('tx', 'ty', 'mem')), may hold values from 0 to 2047
- obs_layer: int32 [262144], P(('tx', 'ty', 'mem')), may hold values from 0 to 11
- obs_tile: int32 [262144], P(('tx', 'ty', 'mem')), may hold values from 0 to 15, as said below
- obs_length: int32 [32], P(('tx', 'ty', 'mem')), may hold values from 4096 to 8192, as said below
- ensemble: bfloat16 [80, 6, 2, 128, 256], P('mem', None, None, 'tx', 'ty'), may hold values from -6 to 6
Outputs:
- alpha_grad: bfloat16 [80, 2, 128, 256], P('mem', None, 'tx', 'ty')
The draws below stay inside these ranges and needn't reach their ends.
Inputs may be any that keep to these rules, and one draw needn't show every extreme that they name: `obs_tile`: among the 8192 entries of one device's list, padding included, at most 1536 name one tile; one tile is named by exactly 1536 live entries of every device's list. `obs_length`: every fourth list is full.
All inputs are finite; a program needn't handle non-finite values.
Results may differ from the reference program's by a relative error of at most 0.001.
Values sent between devices are 32-bit elements; how exact they have to be, the bound alone decides.
A program may use at most 64 MiB of HBM per device.

```python
import jax
import jax.numpy as jnp
from jax import lax

CX = 16
CY = 128
LEV = 2
SLOTS = 6
MEMBERS = 80
OBS_DEV = 8192
TILES = 16
CAP = 1536
LAYERS = 12
NX = 128
NY = 256
NSRC = 32
NOBS = 262144
N_TY = 2


def draw_obs_tile(key, part):
    hot_tile = jax.random.randint(jax.random.fold_in(key, 11), (), 0, TILES)
    popular = jax.random.randint(jax.random.fold_in(key, 12), (TILES,), 0, 2 ** 19)
    slot_tile = jnp.arange(TILES * CAP, dtype=jnp.int32) // CAP

    def one_list(subkey):
        first_key, second_key = jax.random.split(subkey)
        score = jax.random.randint(first_key, (TILES * CAP,), 0, 2 ** 20) + popular[slot_tile]
        score = jnp.where(slot_tile == hot_tile, 2 ** 23, score)
        order = jnp.argsort(score, stable=True)
        others = slot_tile[order[:OBS_DEV - CAP]]
        front = jnp.concatenate([jnp.full((CAP,), hot_tile, jnp.int32), others[:OBS_DEV // 2 - CAP]])
        front = front[jax.random.permutation(second_key, OBS_DEV // 2)]
        return jnp.concatenate([front, others[OBS_DEV // 2 - CAP:]])
    list_keys = jax.random.split(jax.random.fold_in(key, 13), NSRC)
    return jax.vmap(one_list)(list_keys).reshape(NOBS).astype(jnp.int32)


def draw_obs_length(key, part):
    lengths = jax.random.randint(jax.random.fold_in(key, 21), (NSRC,), OBS_DEV // 2, OBS_DEV + 1)
    full_list = jnp.arange(NSRC, dtype=jnp.int32) % 4 == 0
    return jnp.where(full_list, OBS_DEV, lengths).astype(jnp.int32)


def place_ends(drawn, own_key, least, top_value):
    longest = drawn.shape.index(max(drawn.shape))
    spots = []
    for shift in (0, 1):
        where = [jax.random.randint(jax.random.fold_in(own_key, axis), (), 0, length) for axis, length in enumerate(drawn.shape)]
        where[longest] = (where[longest] + shift) % drawn.shape[longest]
        spots.append(tuple(where))
    return drawn.at[spots[0]].set(least).at[spots[1]].set(top_value)


def level_of(rng, extent, shards, low, top_value):
    loudness = 1.0
    for position, blocks in shards:
        draws = jax.random.uniform(jax.random.fold_in(jax.random.fold_in(rng, 6), position), (blocks,), jnp.float32, low / len(shards), top_value / len(shards))
        loudness = loudness * jnp.repeat(jnp.exp(draws), extent[position] // blocks).reshape((-1,) + (1,) * (len(extent) - 1 - position))
    return loudness


def normal_values(key, shape, deviation, limit, shards=(), kind=jnp.bfloat16):
    level = level_of(key, shape, shards, -0.22, 0.18) if shards else 1.0
    values = jax.random.normal(key, shape, jnp.float32) * deviation * level
    return jnp.minimum(jnp.maximum(values, -limit), limit).astype(kind)


def setup_inputs(seed: int = 0) -> dict:
    key_list = jax.random.split(jax.random.key(seed), 8)
    return {
        "obs_value": normal_values(key_list[0], (NOBS,), 1.0, 6.0, ((0, 32),), jnp.float32),
        "obs_frac": jnp.clip(1.0 * jax.random.uniform(key_list[1], (2, NOBS), jnp.float32) ** level_of(key_list[1], (2, NOBS), ((1, 32),), -0.2, 0.2), 0.0, 1.0),
        "obs_cell": place_ends(jax.random.randint(key_list[2], (NOBS,), 0, CX * CY), jax.random.fold_in(key_list[2], 1), 0, (CX * CY) - 1).astype(jnp.int32),
        "obs_layer": place_ends(jax.random.randint(key_list[3], (NOBS,), 0, LAYERS), jax.random.fold_in(key_list[3], 1), 0, LAYERS - 1).astype(jnp.int32),
        "obs_tile": draw_obs_tile(jax.random.fold_in(key_list[7], 71), 0),
        "obs_length": draw_obs_length(jax.random.fold_in(key_list[7], 71), 0),
        "ensemble": normal_values(key_list[6], (MEMBERS, SLOTS, LEV, NX, NY), 1.0, 6.0, ((0, 2), (3, 8), (4, 2))),
    }


def smooth(field):
    padded = jnp.pad(field, ((0, 0), (1, 1), (1, 1)))
    along_x = 0.25 * padded[:, :-2, :] + 0.5 * padded[:, 1:-1, :] + 0.25 * padded[:, 2:, :]
    return 0.25 * along_x[:, :, :-2] + 0.5 * along_x[:, :, 1:-1] + 0.25 * along_x[:, :, 2:]


def reference(obs_value, obs_frac, obs_cell, obs_layer, obs_tile, obs_length, ensemble):
    total = obs_value.shape[0]
    index = jnp.arange(total, dtype=jnp.int32)
    source = index // OBS_DEV
    entry = index % OBS_DEV
    live_rows = entry < obs_length[source]
    base_x = (obs_tile // N_TY) * CX + obs_cell // CY
    base_y = (obs_tile % N_TY) * CY + obs_cell % CY
    frac_x = obs_frac[0]
    frac_y = obs_frac[1]
    grad = jnp.zeros((LAYERS, NX, NY), jnp.float32)
    corners = [(0, 0, (1.0 - frac_x) * (1.0 - frac_y)), (1, 0, frac_x * (1.0 - frac_y)),
               (0, 1, (1.0 - frac_x) * frac_y), (1, 1, frac_x * frac_y)]
    for shift_x, shift_y, weight in corners:
        where_x = base_x + shift_x
        where_y = base_y + shift_y
        inside = live_rows & (where_x < NX) & (where_y < NY)
        amount = jnp.where(inside, obs_value * weight, jnp.float32(0.0))
        grad = grad.at[obs_layer, jnp.minimum(where_x, NX - 1), jnp.minimum(where_y, NY - 1)].add(amount)
    grad_slots = grad.reshape(SLOTS, LEV, NX, NY)

    def member(perturb):
        contrib = jnp.sum(perturb.astype(jnp.float32) * grad_slots, axis=0)
        return smooth(contrib).astype(jnp.bfloat16)

    return lax.map(member, ensemble)
```

```python
import functools

import jax
import jax.numpy as jnp
from jax import lax
from jax.experimental import pallas as pl
from jax.experimental.pallas import tpu as pltpu
from jax.sharding import PartitionSpec as P

MESH = pl.DeviceIdType.MESH
F32 = jnp.float32
BF16 = jnp.bfloat16
LO = 256


def up_to(n, m):
    return (n + m - 1) // m * m


def split(x):
    high = x.astype(BF16)
    low = (x - high.astype(F32)).astype(BF16)
    return high, low


def dot_nt(a, b, precision=None):
    return lax.dot_general(
        a, b, (((1,), (1,)), ((), ())), precision=precision, preferred_element_type=F32
    )


def flat(rows):
    return jnp.concatenate([rows[i : i + 1] for i in range(rows.shape[0])], axis=1)


def hot(ids, code, on):
    return jnp.where(ids == code, on, jnp.zeros((), on.dtype))


def pack_kernel(tiles, hi, cells, value, frac, cell, layer, tile, length, out, acc, code_s, lo_s, val_s, pos_s):
    rows = value.shape[0]
    lanes = 128
    row_id = lax.broadcasted_iota(jnp.int32, (rows, lanes), 0)
    lane_id = lax.broadcasted_iota(jnp.int32, (rows, lanes), 1)
    tile_v = tile[...]
    masks = [jnp.where(tile_v == t, 1.0, 0.0).astype(F32) for t in range(tiles)]
    stacked = jnp.concatenate(masks, axis=0).astype(BF16)
    a = lax.broadcasted_iota(jnp.int32, (lanes, 2 * lanes), 0)
    b = lax.broadcasted_iota(jnp.int32, (lanes, 2 * lanes), 1)
    upper = jnp.where((a <= b) | (b >= lanes), 1.0, 0.0).astype(BF16)
    sums = jnp.dot(stacked, upper, preferred_element_type=F32)
    totals = jnp.concatenate(
        [sums[t * rows : (t + 1) * rows, lanes:] for t in range(tiles)], axis=1
    ).astype(BF16)
    c = lax.broadcasted_iota(jnp.int32, (rows, rows), 0)
    d = lax.broadcasted_iota(jnp.int32, (rows, rows), 1)
    lower = jnp.where(d < c, 1.0, 0.0).astype(BF16)
    offsets = jnp.dot(lower, totals, preferred_element_type=F32)
    rank = jnp.full((rows, lanes), -1.0, F32)
    for t in range(tiles):
        inner = sums[t * rows : (t + 1) * rows, :lanes] + offsets[:, t * lanes : (t + 1) * lanes]
        rank = rank + masks[t] * inner
    rank = rank.astype(jnp.int32)
    code_s[...] = tile_v * hi + rank // LO
    lo_s[...] = rank % LO
    live = row_id * lanes + lane_id < length[0]
    val_s[...] = jnp.where(live, value[...], 0.0)
    pos_s[...] = layer[...] * cells + cell[...]
    acc[...] = jnp.zeros_like(acc)
    step_rows = 8
    width = step_rows * lanes
    groups = tiles * hi
    group_id = lax.broadcasted_iota(jnp.int32, (groups, width), 0)
    lo_id = lax.broadcasted_iota(jnp.int32, (LO, width), 0)
    for s in range(rows // step_rows):
        here = pl.ds(s * step_rows, step_rows)
        along = pl.ds(s * width, width)
        code = flat(code_s[here, :])
        low_hot = jnp.where(lo_id == flat(lo_s[here, :]), 1.0, 0.0).astype(BF16)
        pos = flat(pos_s[here, :])
        pos_low = pos % 128
        fields = [
            split(flat(val_s[here, :])),
            split(frac[0:1, along]),
            split(frac[1:2, along]),
            ((pos - pos_low).astype(F32).astype(BF16), pos_low.astype(F32).astype(BF16)),
        ]
        mine = group_id == code
        for part in range(2):
            left = jnp.concatenate(
                [jnp.where(mine, f[part].astype(F32), 0.0) for f in fields], axis=0
            ).astype(BF16)
            acc[...] += dot_nt(left, low_hot)
    for t in range(tiles):
        for f in range(4):
            start = f * groups + t * hi
            out[t, f * hi : (f + 1) * hi, :] = acc[start : start + hi, :]


def main_kernel(dims, packed, ens, out, recv, acc, acc_in, gt, east_in, north_in, corner_in, con, west_h, east_h,
                send_w, send_e, edge, edge_n, edge_s, ens_v,
                s_send, s_recv, p_sem, rim_send, rim_recv, halo_send, halo_recv, local_sem):
    n_tx, n_ty, n_mem, hi, layers, cx, cy, members, slots, levels = dims
    tiles = n_tx * n_ty
    tx, ty, mem = lax.axis_index("tx"), lax.axis_index("ty"), lax.axis_index("mem")
    me = tx * n_ty + ty
    load = pltpu.make_async_copy(ens, ens_v, local_sem)
    load.start()

    barrier = pltpu.get_barrier_semaphore()

    def greet(k, c):
        t = lax.rem(me + k, tiles)
        pl.semaphore_signal(barrier, inc=1, device_id=(t // n_ty, lax.rem(t, n_ty), mem), device_id_type=MESH)
        return c

    lax.fori_loop(1, tiles, greet, 0)
    partner = (tx, ty, lax.rem(mem + 1, n_mem))
    pl.semaphore_signal(barrier, inc=1, device_id=partner, device_id_type=MESH)
    pl.semaphore_wait(barrier, tiles)

    def copy_to(t):
        return pltpu.make_async_remote_copy(
            src_ref=packed.at[t], dst_ref=recv.at[me], send_sem=s_send.at[t], recv_sem=s_recv.at[me],
            device_id=(t // n_ty, lax.rem(t, n_ty), mem), device_id_type=MESH)

    def send(k, c):
        copy_to(lax.rem(me + k, tiles)).start()
        return c

    lax.fori_loop(1, tiles, send, 0)

    width = hi * LO
    r_rows = up_to(layers * cx + layers, 16)
    y_rows = up_to(cy + 1, 16)
    r_id = lax.broadcasted_iota(jnp.int32, (r_rows, width), 0)
    y_id = lax.broadcasted_iota(jnp.int32, (y_rows, width), 0)
    cells = cx * cy

    def spread(block):
        val, fx, fy, pos = [flat(block[f * hi : (f + 1) * hi]) for f in range(4)]
        pos = pos.astype(jnp.int32)
        lay = pos // cells
        col = pos % cells
        x = col // cy
        y = col % cy
        c1 = lay * cx + x
        c2 = jnp.where(x == cx - 1, layers * cx + lay, c1 + 1)
        left = jnp.where(r_id == c1, val * (1.0 - fx), jnp.where(r_id == c2, val * fx, 0.0))
        right = jnp.where(y_id == y, 1.0 - fy, jnp.where(y_id == y + 1, fy, 0.0))
        lh, ll = split(left)
        rh, rl = split(right)
        acc[0:y_rows, 0:r_rows] += dot_nt(rh, lh) + dot_nt(rl, lh) + dot_nt(rh, ll)

    acc[...] = jnp.zeros_like(acc)
    spread(packed[me])

    def receive(k, c):
        src = lax.rem(me + tiles - k, tiles)
        pltpu.make_async_remote_copy(
            src_ref=packed.at[src], dst_ref=recv.at[src], send_sem=s_send.at[src], recv_sem=s_recv.at[src],
            device_id=(tx, ty, mem), device_id_type=MESH).wait_recv()
        spread(recv[src])
        return c

    lax.fori_loop(1, tiles, receive, 0)

    def drain(k, c):
        copy_to(lax.rem(me + k, tiles)).wait_send()
        return c

    lax.fori_loop(1, tiles, drain, 0)

    swap = pltpu.make_async_remote_copy(
        src_ref=acc.at[pl.ds(0, y_rows)], dst_ref=acc_in, send_sem=p_sem.at[0], recv_sem=p_sem.at[1],
        device_id=partner, device_id_type=MESH)
    swap.start()
    swap.wait()
    acc[0:y_rows, :] += acc_in[...]
    gt[...] = acc[...].T

    east_dev = (lax.rem(tx + 1, n_tx), ty, mem)
    west_dev = (lax.rem(tx + n_tx - 1, n_tx), ty, mem)
    north_dev = (tx, lax.rem(ty + 1, n_ty), mem)
    south_dev = (tx, lax.rem(ty + n_ty - 1, n_ty), mem)
    corner_dev = (lax.rem(tx + 1, n_tx), lax.rem(ty + 1, n_ty), mem)
    rim_rows = pl.ds(layers * cx, 16)
    rims = [
        pltpu.make_async_remote_copy(
            src_ref=s, dst_ref=d, send_sem=rim_send.at[i], recv_sem=rim_recv.at[i], device_id=dev,
            device_id_type=MESH)
        for i, (s, d, dev) in enumerate([
            (gt.at[rim_rows, pl.ds(0, cy)], east_in, east_dev),
            (acc.at[pl.ds(cy, 8)], north_in, north_dev),
            (gt.at[rim_rows, pl.ds(cy, cy)], corner_in, corner_dev),
        ])
    ]
    for c in rims:
        c.start()
    for c in rims:
        c.wait()
    from_west = (tx > 0).astype(F32)
    from_south = (ty > 0).astype(F32)
    north = jnp.concatenate([north_in[...] * from_south, jnp.zeros((cy - 8, north_in.shape[1]), F32)], axis=0)
    grad = gt[0 : layers * cx, 0:cy] + north.T[0 : layers * cx]
    east = (east_in[...] + corner_in[...] * from_south) * from_west
    x_id = lax.broadcasted_iota(jnp.int32, (cx, cy), 0)
    g = [
        grad[k * cx : (k + 1) * cx] + jnp.where(x_id == 0, east[k : k + 1], 0.0)
        for k in range(layers)
    ]
    load.wait()

    def contract(m, c):
        for l in range(levels):
            total = jnp.zeros((cx, cy), F32)
            for t in range(slots):
                total = total + ens_v[m, t, l].astype(F32) * g[t * levels + l]
            con[m * levels + l] = total
            send_w[pl.ds(m * levels + l, 1), :] = total[0:1]
            send_e[pl.ds(m * levels + l, 1), :] = total[cx - 1 : cx]
        return c

    lax.fori_loop(0, members, contract, 0)

    halos = [
        pltpu.make_async_remote_copy(
            src_ref=s, dst_ref=d, send_sem=halo_send.at[i], recv_sem=halo_recv.at[i], device_id=dev,
            device_id_type=MESH)
        for i, (s, d, dev) in enumerate([(send_w, east_h, west_dev), (send_e, west_h, east_dev)])
    ]
    for c in halos:
        c.start()
    for c in halos:
        c.wait()
    to_east = (tx < n_tx - 1).astype(F32)
    to_north = (ty < n_ty - 1).astype(F32)

    def filter_x(i, c):
        mid = con[i]
        before = jnp.where(x_id == 0, west_h[pl.ds(i, 1), :] * from_west, pltpu.roll(mid, 1, 0))
        after = jnp.where(x_id == cx - 1, east_h[pl.ds(i, 1), :] * to_east, pltpu.roll(mid, cx - 1, 0))
        con[i] = 0.25 * before + 0.5 * mid + 0.25 * after
        return c

    planes = members * levels
    lax.fori_loop(0, planes, filter_x, 0)
    e_row = lax.broadcasted_iota(jnp.int32, (8, cy), 0)
    e_lane = lax.broadcasted_iota(jnp.int32, (8, cy), 1)
    pick = jnp.where((e_row == 0) & (e_lane == 0) | (e_row == 1) & (e_lane == cy - 1), 1.0, 0.0)
    edge[...] = dot_nt(pick, con[...].reshape(planes * cx, cy), lax.Precision.HIGHEST)
    up = pltpu.make_async_remote_copy(
        src_ref=edge, dst_ref=edge_s, send_sem=halo_send.at[2], recv_sem=halo_recv.at[2],
        device_id=north_dev, device_id_type=MESH)
    both = [up]
    if n_ty > 2:
        both.append(pltpu.make_async_remote_copy(
            src_ref=edge, dst_ref=edge_n, send_sem=halo_send.at[3], recv_sem=halo_recv.at[3],
            device_id=south_dev, device_id_type=MESH))
    for c in both:
        c.start()
    for c in both:
        c.wait()
    south_row = jnp.where((e_row == 1) & (e_lane == 0), 0.25 * from_south, 0.0)
    north_row = jnp.where((e_row == 0) & (e_lane == cy - 1), 0.25 * to_north, 0.0)

    def outer(e, place):
        return lax.dot_general(e, place, (((0,), (0,)), ((), ())), precision=lax.Precision.HIGHEST,
                               preferred_element_type=F32)

    if n_ty == 2:
        fix = outer(edge_s[...], south_row + north_row)
    else:
        fix = outer(edge_s[...], south_row) + outer(edge_n[...], north_row)
    lane = lax.broadcasted_iota(jnp.int32, (planes * cx, cy), 1)
    mid = con[...].reshape(planes * cx, cy)
    left = jnp.where(lane == 0, 0.0, pltpu.roll(mid, 1, 1))
    right = jnp.where(lane == cy - 1, 0.0, pltpu.roll(mid, cy - 1, 1))
    res = 0.25 * left + 0.5 * mid + 0.25 * right + fix
    out[...] = res.astype(BF16).reshape(out.shape)


def body(mesh_sizes, obs_value, obs_frac, obs_cell, obs_layer, obs_tile, obs_length, ensemble):
    n_tx, n_ty, n_mem = mesh_sizes
    tiles = n_tx * n_ty
    count = obs_value.shape[0]
    hi = pl.cdiv(3 * count // tiles, LO)
    members, slots, levels, cx, cy = ensemble.shape
    layers = slots * levels
    vmem = pl.BlockSpec(memory_space=pltpu.VMEM)
    smem = pl.BlockSpec(memory_space=pltpu.SMEM)
    rows = count // 128
    packed = pl.pallas_call(
        functools.partial(pack_kernel, tiles, hi, cx * cy),
        out_shape=jax.ShapeDtypeStruct((tiles, 4 * hi, LO), F32),
        in_specs=[vmem] * 5 + [smem],
        out_specs=vmem,
        scratch_shapes=[
            pltpu.VMEM((4 * tiles * hi, LO), F32),
            pltpu.VMEM((rows, 128), jnp.int32),
            pltpu.VMEM((rows, 128), jnp.int32),
            pltpu.VMEM((rows, 128), F32),
            pltpu.VMEM((rows, 128), jnp.int32),
        ],
    )(obs_value.reshape(rows, 128), obs_frac, obs_cell.reshape(rows, 128), obs_layer.reshape(rows, 128),
      obs_tile.reshape(rows, 128), obs_length)

    planes = members * levels
    y_rows = up_to(cy + 1, 16)
    square = 2 * cy
    dma = pltpu.SemaphoreType.DMA
    scratch = [
        pltpu.VMEM((tiles, 4 * hi, LO), F32),
        pltpu.VMEM((square, square), F32),
        pltpu.VMEM((y_rows, square), F32),
        pltpu.VMEM((square, square), F32),
        pltpu.VMEM((16, cy), F32),
        pltpu.VMEM((8, square), F32),
        pltpu.VMEM((16, cy), F32),
        pltpu.VMEM((planes, cx, cy), F32),
        pltpu.VMEM((planes, cy), F32),
        pltpu.VMEM((planes, cy), F32),
        pltpu.VMEM((planes, cy), F32),
        pltpu.VMEM((planes, cy), F32),
        pltpu.VMEM((8, planes * cx), F32),
        pltpu.VMEM((8, planes * cx), F32),
        pltpu.VMEM((8, planes * cx), F32),
        pltpu.VMEM(ensemble.shape, BF16),
        dma((tiles,)), dma((tiles,)), dma((2,)), dma((3,)), dma((3,)), dma((4,)), dma((4,)), dma,
    ]
    dims = (n_tx, n_ty, n_mem, hi, layers, cx, cy, members, slots, levels)
    return pl.pallas_call(
        functools.partial(main_kernel, dims),
        out_shape=jax.ShapeDtypeStruct((members, levels, cx, cy), BF16),
        in_specs=[vmem, pl.BlockSpec(memory_space=pl.ANY)],
        out_specs=vmem,
        scratch_shapes=scratch,
        compiler_params=pltpu.CompilerParams(collective_id=0, has_side_effects=True),
    )(packed, ensemble)


def solution(mesh):
    placed = (
        P(("tx", "ty", "mem")),
        P(None, ("tx", "ty", "mem")),
        P(("tx", "ty", "mem")),
        P(("tx", "ty", "mem")),
        P(("tx", "ty", "mem")),
        P(("tx", "ty", "mem")),
        P("mem", None, None, "tx", "ty"),
    )
    sizes = tuple(mesh.shape[a] for a in ("tx", "ty", "mem"))
    return jax.shard_map(
        functools.partial(body, sizes), mesh=mesh, in_specs=placed, out_specs=P("mem", None, "tx", "ty"),
        check_vma=False,
    )
```

```python
import functools

import jax
import jax.numpy as jnp
from jax import lax
from jax.experimental import pallas as pl
from jax.experimental.pallas import tpu as pltpu
from jax.sharding import PartitionSpec as P

MESH = pl.DeviceIdType.MESH
F32 = jnp.float32
BF16 = jnp.bfloat16
LO = 256


def up_to(n, m):
    return (n + m - 1) // m * m


def split(x):
    high = x.astype(BF16)
    low = (x - high.astype(F32)).astype(BF16)
    return high, low


def dot_nt(a, b, precision=None):
    return lax.dot_general(
        a, b, (((1,), (1,)), ((), ())), precision=precision, preferred_element_type=F32
    )


def flat(rows):
    return jnp.concatenate([rows[i : i + 1] for i in range(rows.shape[0])], axis=1)


def strip(x):
    parts = [
        jnp.broadcast_to(x[i : i + 1], (16, x.shape[1])).astype(BF16) for i in range(x.shape[0])
    ]
    return jnp.concatenate(parts, axis=1)


def tall(x, rows):
    return jnp.concatenate([x] * (rows // 16), axis=0)


def ids(rows, width):
    return lax.broadcasted_iota(jnp.int32, (rows, 128), 0).astype(F32).astype(BF16), width // 128


def wide_ids(rows, width):
    base, times = ids(rows, width)
    return jnp.concatenate([base] * times, axis=1)


def parts_of(x):
    high = x.astype(BF16).astype(F32)
    return strip(high), strip(x - high)


def pick_two(number, first, second, on_first, on_second):
    rows = number.shape[0]
    zero = jnp.zeros((), BF16)
    inner = jnp.where(number == tall(second, rows), tall(on_second, rows), zero)
    return jnp.where(number == tall(first, rows), tall(on_first, rows), inner)


def shift_mix(x, axis, ids_along):
    size = x.shape[axis]
    before = jnp.where(ids_along == 0, 0.0, pltpu.roll(x, 1, axis))
    after = jnp.where(ids_along == size - 1, 0.0, pltpu.roll(x, size - 1, axis))
    return 0.25 * before + 0.5 * x + 0.25 * after


def pack_kernel(tiles, hi, cells, value, frac, cell, layer, tile, length, out, acc, code_s, lo_s, val_s, pos_s):
    rows = value.shape[0]
    lanes = 128
    row_id = lax.broadcasted_iota(jnp.int32, (rows, lanes), 0)
    lane_id = lax.broadcasted_iota(jnp.int32, (rows, lanes), 1)
    tile_v = tile[...]
    masks = [jnp.where(tile_v == t, 1.0, 0.0).astype(F32) for t in range(tiles)]
    stacked = jnp.concatenate(masks, axis=0).astype(BF16)
    a = lax.broadcasted_iota(jnp.int32, (lanes, 2 * lanes), 0)
    b = lax.broadcasted_iota(jnp.int32, (lanes, 2 * lanes), 1)
    upper = jnp.where((a <= b) | (b >= lanes), 1.0, 0.0).astype(BF16)
    sums = jnp.dot(stacked, upper, preferred_element_type=F32)
    totals = jnp.concatenate(
        [sums[t * rows : (t + 1) * rows, lanes:] for t in range(tiles)], axis=1
    ).astype(BF16)
    c = lax.broadcasted_iota(jnp.int32, (rows, rows), 0)
    d = lax.broadcasted_iota(jnp.int32, (rows, rows), 1)
    lower = jnp.where(d < c, 1.0, 0.0).astype(BF16)
    offsets = jnp.dot(lower, totals, preferred_element_type=F32)
    rank = jnp.full((rows, lanes), -1.0, F32)
    for t in range(tiles):
        inner = sums[t * rows : (t + 1) * rows, :lanes] + offsets[:, t * lanes : (t + 1) * lanes]
        rank = rank + masks[t] * inner
    rank = rank.astype(jnp.int32)
    code_s[...] = tile_v * hi + rank // LO
    lo_s[...] = rank % LO
    live = row_id * lanes + lane_id < length[0]
    val_s[...] = jnp.where(live, value[...], 0.0)
    pos_s[...] = layer[...] * cells + cell[...]
    acc[...] = jnp.zeros_like(acc)
    step_rows = 8
    width = step_rows * lanes
    groups = tiles * hi
    group_id = wide_ids(up_to(groups, 16), width)
    lo_id = wide_ids(LO, width)
    one = jnp.ones((), BF16)
    zero = jnp.zeros((), BF16)
    for s in range(rows // step_rows):
        here = pl.ds(s * step_rows, step_rows)
        along = pl.ds(s * width, width)
        code = tall(strip(code_s[here, :].astype(F32)), groups)
        low = tall(strip(lo_s[here, :].astype(F32)), LO)
        low_hot = jnp.where(lo_id == low, one, zero)
        pos = pos_s[here, :]
        pos_low = pos % 128
        fields = [
            parts_of(val_s[here, :]),
            parts_of(frac[0:1, along]),
            parts_of(frac[1:2, along]),
            (strip((pos - pos_low).astype(F32)), strip(pos_low.astype(F32))),
        ]
        mine = group_id == code
        for part in range(2):
            left = jnp.concatenate(
                [jnp.where(mine, tall(f[part], groups), zero) for f in fields], axis=0
            )
            acc[...] += dot_nt(left, low_hot)
    for t in range(tiles):
        for f in range(4):
            start = f * groups + t * hi
            out[t, f * hi : (f + 1) * hi, :] = acc[start : start + hi, :]


def main_kernel(dims, packed, ens, out, recv, acc, acc_in, gt, east_in, north_in, corner_in, con, fix, west_h, east_h,
                send_w, send_e, edge, edge_in, corner_w, corner_e, corner_from_e, corner_from_w, ens_v,
                s_send, s_recv, p_sem, rim_send, rim_recv, halo_send, halo_recv, local_sem):
    n_tx, n_ty, n_mem, hi, layers, cx, cy, members, slots, levels = dims
    tiles = n_tx * n_ty
    tx, ty, mem = lax.axis_index("tx"), lax.axis_index("ty"), lax.axis_index("mem")
    me = tx * n_ty + ty
    load = pltpu.make_async_copy(ens, ens_v, local_sem)
    load.start()
    has_west, has_east = tx > 0, tx < n_tx - 1
    has_south, has_north = ty > 0, ty < n_ty - 1

    barrier = pltpu.get_barrier_semaphore()
    total_devices = tiles * n_mem
    my_id = me * n_mem + mem

    def greet(k, c):
        d = lax.rem(my_id + k, total_devices)
        t = d // n_mem
        pl.semaphore_signal(barrier, inc=1, device_id=(t // n_ty, lax.rem(t, n_ty), lax.rem(d, n_mem)),
                            device_id_type=MESH)
        return c

    lax.fori_loop(1, total_devices, greet, 0)
    partner = (tx, ty, lax.rem(mem + 1, n_mem))
    pl.semaphore_wait(barrier, total_devices - 1)

    def copy_to(t):
        return pltpu.make_async_remote_copy(
            src_ref=packed.at[t], dst_ref=recv.at[me], send_sem=s_send.at[t], recv_sem=s_recv.at[me],
            device_id=(t // n_ty, lax.rem(t, n_ty), mem), device_id_type=MESH)

    def send(k, c):
        copy_to(lax.rem(me + k, tiles)).start()
        return c

    lax.fori_loop(1, tiles, send, 0)

    width = hi * LO
    r_rows = up_to(layers * cx + layers, 16)
    y_rows = up_to(cy + 1, 16)
    r_id = wide_ids(r_rows, width)
    y_id = wide_ids(y_rows, width)
    cells = cx * cy

    def spread(block):
        val, fx, fy, pos = [block[f * hi : (f + 1) * hi] for f in range(4)]
        pos = pos.astype(jnp.int32)
        lay = pos // cells
        col = pos % cells
        x = col // cy
        y = (col % cy).astype(F32)
        c1 = lay * cx + x
        c2 = jnp.where(x == cx - 1, layers * cx + lay, c1 + 1)
        c1, c2 = strip(c1.astype(F32)), strip(c2.astype(F32))
        y1, y2 = strip(y), strip(y + 1.0)
        near, far = parts_of(val * (1.0 - fx)), parts_of(val * fx)
        low, high = parts_of(1.0 - fy), parts_of(fy)
        lh, ll = [pick_two(r_id, c1, c2, near[i], far[i]) for i in range(2)]
        rh, rl = [pick_two(y_id, y1, y2, low[i], high[i]) for i in range(2)]
        acc[0:y_rows, 0:r_rows] += dot_nt(rh, lh) + dot_nt(rl, lh) + dot_nt(rh, ll)

    acc[...] = jnp.zeros_like(acc)

    @pl.when(jnp.logical_not(has_west))
    def _():
        east_in[...] = jnp.zeros_like(east_in)
        west_h[...] = jnp.zeros_like(west_h)

    @pl.when(jnp.logical_not(has_east))
    def _():
        east_h[...] = jnp.zeros_like(east_h)

    @pl.when(jnp.logical_not(has_south))
    def _():
        north_in[...] = jnp.zeros_like(north_in)

    @pl.when(jnp.logical_not(has_south & has_west))
    def _():
        corner_in[...] = jnp.zeros_like(corner_in)

    spread(packed[me])

    def receive(k, c):
        src = lax.rem(me + tiles - k, tiles)
        pltpu.make_async_remote_copy(
            src_ref=packed.at[src], dst_ref=recv.at[src], send_sem=s_send.at[src], recv_sem=s_recv.at[src],
            device_id=partner, device_id_type=MESH).wait_recv()
        spread(recv[src])
        return c

    lax.fori_loop(1, tiles, receive, 0)

    swap = pltpu.make_async_remote_copy(
        src_ref=acc.at[pl.ds(0, y_rows)], dst_ref=acc_in, send_sem=p_sem.at[0], recv_sem=p_sem.at[1],
        device_id=partner, device_id_type=MESH)
    swap.start()

    def remote(src, dst, send_sem, recv_sem, dev):
        return pltpu.make_async_remote_copy(src_ref=src, dst_ref=dst, send_sem=send_sem, recv_sem=recv_sem,
                                            device_id=dev, device_id_type=MESH)

    def start(copies):
        for c, sends, _ in copies:
            pl.when(sends)(c.start)

    def finish(copies):
        for c, sends, gets in copies:
            pl.when(gets)(c.wait_recv)
            pl.when(sends)(c.wait_send)

    e_tx, w_tx = lax.rem(tx + 1, n_tx), lax.rem(tx + n_tx - 1, n_tx)
    n_ty_id, s_ty_id = lax.rem(ty + 1, n_ty), lax.rem(ty + n_ty - 1, n_ty)
    rim_rows = pl.ds(layers * cx, 16)
    rims = []
    for q in range(n_mem):
        other = lax.rem(mem + q, n_mem)
        rims.append((remote(acc.at[pl.ds(cy, 8)], north_in.at[q], rim_send.at[0, q], rim_recv.at[0, q],
                            (tx, n_ty_id, other)), has_north, has_south))
    start(rims)
    gt[...] = acc[...].T
    late = []
    for q in range(n_mem):
        other = lax.rem(mem + q, n_mem)
        late.append((remote(gt.at[rim_rows, pl.ds(0, cy)], east_in.at[q], rim_send.at[1, q], rim_recv.at[1, q],
                            (e_tx, ty, other)), has_east, has_west))
        late.append((remote(gt.at[rim_rows, pl.ds(cy, cy)], corner_in.at[q], rim_send.at[2, q], rim_recv.at[2, q],
                            (e_tx, n_ty_id, other)), has_east & has_north, has_west & has_south))
    start(late)

    def drain(k, c):
        copy_to(lax.rem(me + k, tiles)).wait_send()
        return c

    lax.fori_loop(1, tiles, drain, 0)
    swap.wait()
    joined = jnp.concatenate([acc_in[...], jnp.zeros((2 * cy - y_rows, acc_in.shape[1]), F32)], axis=0).T
    grad = gt[0 : layers * cx, 0:cy] + joined[0 : layers * cx, 0:cy]
    finish(rims + late)
    north = sum(north_in[q] for q in range(n_mem))
    north = jnp.concatenate([north, jnp.zeros((cy - 8, north.shape[1]), F32)], axis=0)
    grad = grad + north.T[0 : layers * cx]
    east = sum(east_in[q] + corner_in[q] for q in range(n_mem))
    x_id = lax.broadcasted_iota(jnp.int32, (cx, cy), 0)
    g = [
        grad[k * cx : (k + 1) * cx] + jnp.where(x_id == 0, east[k : k + 1], 0.0)
        for k in range(layers)
    ]
    load.wait()

    def contract(m, c):
        for l in range(levels):
            total = jnp.zeros((cx, cy), F32)
            for t in range(slots):
                total = total + ens_v[m, t, l].astype(F32) * g[t * levels + l]
            con[m * levels + l] = total
            send_w[pl.ds(m * levels + l, 1), :] = total[0:1]
            send_e[pl.ds(m * levels + l, 1), :] = total[cx - 1 : cx]
        return c

    lax.fori_loop(0, members, contract, 0, unroll=2)

    def halo(i, src, dst, dev, sends, gets):
        return (remote(src, dst, halo_send.at[i], halo_recv.at[i], dev), sends, gets)

    sides = [halo(0, send_w, east_h, (w_tx, ty, mem), has_west, has_east),
             halo(1, send_e, west_h, (e_tx, ty, mem), has_east, has_west)]
    start(sides)
    planes = members * levels
    e_row = lax.broadcasted_iota(jnp.int32, (8, cy), 0)
    e_lane = lax.broadcasted_iota(jnp.int32, (8, cy), 1)
    pick = jnp.where((e_row == 0) & (e_lane == 0) | (e_row == 1) & (e_lane == cy - 1), 1.0, 0.0)
    exact = lax.Precision.HIGHEST
    corner_w[...] = dot_nt(pick, send_w[...], exact)
    corner_e[...] = dot_nt(pick, send_e[...], exact)
    edge[...] = dot_nt(pick, con[...].reshape(planes * cx, cy), exact)
    south = jnp.where((e_row == 1) & (e_lane == 0) & has_south, 0.25, 0.0)
    north = jnp.where((e_row == 0) & (e_lane == cy - 1) & has_north, 0.25, 0.0)
    always = tx >= 0
    places = [south + north] if n_ty == 2 else [south, north]
    targets = [n_ty_id, s_ty_id][: len(places)]
    for i, t in enumerate(targets):
        sides += [
            halo(2 + 3 * i, edge, edge_in.at[i], (tx, t, mem), always, always),
            halo(3 + 3 * i, corner_w, corner_from_e.at[i], (w_tx, t, mem), has_west, has_east),
            halo(4 + 3 * i, corner_e, corner_from_w.at[i], (e_tx, t, mem), has_east, has_west),
        ]
        pl.when(jnp.logical_not(has_east))(functools.partial(fill, corner_from_e, i))
        pl.when(jnp.logical_not(has_west))(functools.partial(fill, corner_from_w, i))
    start(sides[2:])

    batch = max(b for b in range(1, 11) if planes % b == 0)
    lane = lax.broadcasted_iota(jnp.int32, (batch * cx, cy), 1)
    x_in = lax.broadcasted_iota(jnp.int32, (batch * cx, cy), 0) % cx

    def local(i, c):
        here = pl.ds(i * batch, batch)
        mid = shift_mix(con[here].reshape(batch * cx, cy), 1, lane)
        before = jnp.where(x_in == 0, 0.0, pltpu.roll(mid, 1, 0))
        after = jnp.where(x_in == cx - 1, 0.0, pltpu.roll(mid, batch * cx - 1, 0))
        con[here] = (0.25 * before + 0.5 * mid + 0.25 * after).reshape(batch, cx, cy)
        return c

    lax.fori_loop(0, planes // batch, local, 0)
    finish(sides)

    def outer(e, place):
        return lax.dot_general(e, place, (((0,), (0,)), ((), ())), precision=exact, preferred_element_type=F32)

    l_in = lax.broadcasted_iota(jnp.int32, (8, planes * cx), 1) % cx
    row_lane = lax.broadcasted_iota(jnp.int32, (planes, cy), 1)
    west = shift_mix(west_h[...], 1, row_lane)
    east = shift_mix(east_h[...], 1, row_lane)
    added = jnp.zeros((planes * cx, cy), F32)
    for i, place in enumerate(places):
        e = edge_in[i]
        before = jnp.where(l_in == 0, 0.0, pltpu.roll(e, 1, 1))
        after = jnp.where(l_in == cx - 1, 0.0, pltpu.roll(e, planes * cx - 1, 1))
        added = added + outer(0.25 * before + 0.5 * e + 0.25 * after, place)
        west = west + outer(corner_from_w[i], place)
        east = east + outer(corner_from_e[i], place)
    fix[...] = added.reshape(planes, cx, cy)
    west_h[...] = 0.25 * west
    east_h[...] = 0.25 * east

    def last(m, c):
        for l in range(levels):
            i = m * levels + l
            res = con[i] + fix[i]
            res = res + jnp.where(x_id == 0, west_h[pl.ds(i, 1), :], 0.0)
            res = res + jnp.where(x_id == cx - 1, east_h[pl.ds(i, 1), :], 0.0)
            out[m, l] = res.astype(BF16)
        return c

    lax.fori_loop(0, members, last, 0, unroll=2)


def fill(ref, i):
    ref[i] = jnp.zeros(ref.shape[1:], F32)


def body(mesh_sizes, obs_value, obs_frac, obs_cell, obs_layer, obs_tile, obs_length, ensemble):
    n_tx, n_ty, n_mem = mesh_sizes
    tiles = n_tx * n_ty
    count = obs_value.shape[0]
    hi = pl.cdiv(3 * count // tiles, LO)
    members, slots, levels, cx, cy = ensemble.shape
    layers = slots * levels
    vmem = pl.BlockSpec(memory_space=pltpu.VMEM)
    smem = pl.BlockSpec(memory_space=pltpu.SMEM)
    rows = count // 128
    packed = pl.pallas_call(
        functools.partial(pack_kernel, tiles, hi, cx * cy),
        out_shape=jax.ShapeDtypeStruct((tiles, 4 * hi, LO), F32),
        in_specs=[vmem] * 5 + [smem],
        out_specs=vmem,
        scratch_shapes=[
            pltpu.VMEM((4 * tiles * hi, LO), F32),
            pltpu.VMEM((rows, 128), jnp.int32),
            pltpu.VMEM((rows, 128), jnp.int32),
            pltpu.VMEM((rows, 128), F32),
            pltpu.VMEM((rows, 128), jnp.int32),
        ],
    )(obs_value.reshape(rows, 128), obs_frac, obs_cell.reshape(rows, 128), obs_layer.reshape(rows, 128),
      obs_tile.reshape(rows, 128), obs_length)

    planes = members * levels
    y_rows = up_to(cy + 1, 16)
    square = 2 * cy
    sides = 1 if n_ty == 2 else 2
    dma = pltpu.SemaphoreType.DMA
    scratch = [
        pltpu.VMEM((tiles, 4 * hi, LO), F32),
        pltpu.VMEM((square, square), F32),
        pltpu.VMEM((y_rows, square), F32),
        pltpu.VMEM((square, square), F32),
        pltpu.VMEM((n_mem, 16, cy), F32),
        pltpu.VMEM((n_mem, 8, square), F32),
        pltpu.VMEM((n_mem, 16, cy), F32),
        pltpu.VMEM((planes, cx, cy), F32),
        pltpu.VMEM((planes, cx, cy), F32),
        pltpu.VMEM((planes, cy), F32),
        pltpu.VMEM((planes, cy), F32),
        pltpu.VMEM((planes, cy), F32),
        pltpu.VMEM((planes, cy), F32),
        pltpu.VMEM((8, planes * cx), F32),
        pltpu.VMEM((sides, 8, planes * cx), F32),
        pltpu.VMEM((8, planes), F32),
        pltpu.VMEM((8, planes), F32),
        pltpu.VMEM((sides, 8, planes), F32),
        pltpu.VMEM((sides, 8, planes), F32),
        pltpu.VMEM(ensemble.shape, BF16),
        dma((tiles,)), dma((tiles,)), dma((2,)), dma((3, n_mem)), dma((3, n_mem)),
        dma((2 + 3 * sides,)), dma((2 + 3 * sides,)), dma,
    ]
    dims = (n_tx, n_ty, n_mem, hi, layers, cx, cy, members, slots, levels)
    return pl.pallas_call(
        functools.partial(main_kernel, dims),
        out_shape=jax.ShapeDtypeStruct((members, levels, cx, cy), BF16),
        in_specs=[vmem, pl.BlockSpec(memory_space=pl.ANY)],
        out_specs=vmem,
        scratch_shapes=scratch,
        compiler_params=pltpu.CompilerParams(collective_id=0, has_side_effects=True),
    )(packed, ensemble)


def solution(mesh):
    placed = (
        P(("tx", "ty", "mem")),
        P(None, ("tx", "ty", "mem")),
        P(("tx", "ty", "mem")),
        P(("tx", "ty", "mem")),
        P(("tx", "ty", "mem")),
        P(("tx", "ty", "mem")),
        P("mem", None, None, "tx", "ty"),
    )
    sizes = tuple(mesh.shape[a] for a in ("tx", "ty", "mem"))
    return jax.shard_map(
        functools.partial(body, sizes), mesh=mesh, in_specs=placed, out_specs=P("mem", None, "tx", "ty"),
        check_vma=False,
    )
```

```python
import functools

import jax
import jax.numpy as jnp
from jax import lax
from jax.experimental import pallas as pl
from jax.experimental.pallas import tpu as pltpu
from jax.sharding import PartitionSpec as P

MESH = pl.DeviceIdType.MESH
F32 = jnp.float32
BF16 = jnp.bfloat16
LO = 256


def up_to(n, m):
    return (n + m - 1) // m * m


def split(x):
    high = x.astype(BF16)
    low = (x - high.astype(F32)).astype(BF16)
    return high, low


def dot_nt(a, b, precision=None):
    return lax.dot_general(
        a, b, (((1,), (1,)), ((), ())), precision=precision, preferred_element_type=F32
    )


def flat(rows):
    return jnp.concatenate([rows[i : i + 1] for i in range(rows.shape[0])], axis=1)


def strip(x):
    parts = [
        jnp.broadcast_to(x[i : i + 1], (16, x.shape[1])).astype(BF16) for i in range(x.shape[0])
    ]
    return jnp.concatenate(parts, axis=1)


def tall(x, rows):
    return jnp.concatenate([x] * (rows // 16), axis=0)


def ids(rows, width):
    return lax.broadcasted_iota(jnp.int32, (rows, 128), 0).astype(F32).astype(BF16), width // 128


def wide_ids(rows, width):
    base, times = ids(rows, width)
    return jnp.concatenate([base] * times, axis=1)


def parts_of(x):
    high = x.astype(BF16).astype(F32)
    return strip(high), strip(x - high)


def pick_two(number, first, second, on_first, on_second):
    rows = number.shape[0]
    zero = jnp.zeros((), BF16)
    inner = jnp.where(number == tall(second, rows), tall(on_second, rows), zero)
    return jnp.where(number == tall(first, rows), tall(on_first, rows), inner)


def shift_mix(x, axis, ids_along):
    size = x.shape[axis]
    before = jnp.where(ids_along == 0, 0.0, pltpu.roll(x, 1, axis))
    after = jnp.where(ids_along == size - 1, 0.0, pltpu.roll(x, size - 1, axis))
    return 0.25 * before + 0.5 * x + 0.25 * after


def pack_kernel(tiles, hi, cells, value, frac, cell, layer, tile, length, out, acc, code_s, lo_s, val_s, pos_s):
    rows = value.shape[0]
    lanes = 128
    row_id = lax.broadcasted_iota(jnp.int32, (rows, lanes), 0)
    lane_id = lax.broadcasted_iota(jnp.int32, (rows, lanes), 1)
    tile_v = tile[...]
    masks = [jnp.where(tile_v == t, 1.0, 0.0).astype(F32) for t in range(tiles)]
    stacked = jnp.concatenate(masks, axis=0).astype(BF16)
    a = lax.broadcasted_iota(jnp.int32, (lanes, 2 * lanes), 0)
    b = lax.broadcasted_iota(jnp.int32, (lanes, 2 * lanes), 1)
    upper = jnp.where((a <= b) | (b >= lanes), 1.0, 0.0).astype(BF16)
    sums = jnp.dot(stacked, upper, preferred_element_type=F32)
    totals = jnp.concatenate(
        [sums[t * rows : (t + 1) * rows, lanes:] for t in range(tiles)], axis=1
    ).astype(BF16)
    c = lax.broadcasted_iota(jnp.int32, (rows, rows), 0)
    d = lax.broadcasted_iota(jnp.int32, (rows, rows), 1)
    lower = jnp.where(d < c, 1.0, 0.0).astype(BF16)
    offsets = jnp.dot(lower, totals, preferred_element_type=F32)
    rank = jnp.full((rows, lanes), -1.0, F32)
    for t in range(tiles):
        inner = sums[t * rows : (t + 1) * rows, :lanes] + offsets[:, t * lanes : (t + 1) * lanes]
        rank = rank + masks[t] * inner
    rank = rank.astype(jnp.int32)
    code_s[...] = tile_v * hi + rank // LO
    lo_s[...] = rank % LO
    live = row_id * lanes + lane_id < length[0]
    val_s[...] = jnp.where(live, value[...], 0.0)
    pos_s[...] = layer[...] * cells + cell[...]
    acc[...] = jnp.zeros_like(acc)
    step_rows = 8
    width = step_rows * lanes
    groups = tiles * hi
    group_id = wide_ids(up_to(groups, 16), width)
    lo_id = wide_ids(LO, width)
    one = jnp.ones((), BF16)
    zero = jnp.zeros((), BF16)
    for s in range(rows // step_rows):
        here = pl.ds(s * step_rows, step_rows)
        along = pl.ds(s * width, width)
        code = tall(strip(code_s[here, :].astype(F32)), groups)
        low = tall(strip(lo_s[here, :].astype(F32)), LO)
        low_hot = jnp.where(lo_id == low, one, zero)
        pos = pos_s[here, :]
        pos_low = pos % 128
        fields = [
            parts_of(val_s[here, :]),
            parts_of(frac[0:1, along]),
            parts_of(frac[1:2, along]),
            (strip((pos - pos_low).astype(F32)), strip(pos_low.astype(F32))),
        ]
        mine = group_id == code
        left = jnp.concatenate(
            [jnp.where(mine, tall(f[part], groups), zero) for part in range(2) for f in fields], axis=0
        )
        both = dot_nt(left, low_hot)
        acc[...] += both[: 4 * groups] + both[4 * groups :]
    for t in range(tiles):
        for f in range(4):
            start = f * groups + t * hi
            out[t, f * hi : (f + 1) * hi, :] = acc[start : start + hi, :]


def main_kernel(dims, packed, ens, out, recv, acc, acc_in, gt, east_in, north_in, corner_in, con, fix, west_h, east_h,
                send_w, send_e, edge, edge_in, corner_w, corner_e, corner_from_e, corner_from_w, ens_v,
                s_send, s_recv, p_sem, rim_send, rim_recv, halo_send, halo_recv, local_sem):
    n_tx, n_ty, n_mem, hi, layers, cx, cy, members, slots, levels = dims
    tiles = n_tx * n_ty
    tx, ty, mem = lax.axis_index("tx"), lax.axis_index("ty"), lax.axis_index("mem")
    me = tx * n_ty + ty
    load = pltpu.make_async_copy(ens, ens_v, local_sem)
    load.start()
    has_west, has_east = tx > 0, tx < n_tx - 1
    has_south, has_north = ty > 0, ty < n_ty - 1

    barrier = pltpu.get_barrier_semaphore()
    total_devices = tiles * n_mem
    my_id = me * n_mem + mem

    def greet(k, c):
        d = lax.rem(my_id + k, total_devices)
        t = d // n_mem
        pl.semaphore_signal(barrier, inc=1, device_id=(t // n_ty, lax.rem(t, n_ty), lax.rem(d, n_mem)),
                            device_id_type=MESH)
        return c

    lax.fori_loop(1, total_devices, greet, 0)
    partner = (tx, ty, lax.rem(mem + 1, n_mem))
    pl.semaphore_wait(barrier, total_devices - 1)

    def copy_to(t):
        return pltpu.make_async_remote_copy(
            src_ref=packed.at[t], dst_ref=recv.at[me], send_sem=s_send.at[t], recv_sem=s_recv.at[me],
            device_id=(t // n_ty, lax.rem(t, n_ty), mem), device_id_type=MESH)

    def send(k, c):
        copy_to(lax.rem(me + k, tiles)).start()
        return c

    lax.fori_loop(1, tiles, send, 0)

    width = hi * LO
    r_rows = up_to(layers * cx + layers, 16)
    y_rows = up_to(cy + 1, 16)
    r_id = wide_ids(r_rows, width)
    y_id = wide_ids(y_rows, width)
    cells = cx * cy

    def spread(block):
        val, fx, fy, pos = [block[f * hi : (f + 1) * hi] for f in range(4)]
        pos = pos.astype(jnp.int32)
        lay = pos // cells
        col = pos % cells
        x = col // cy
        y = (col % cy).astype(F32)
        c1 = lay * cx + x
        c2 = jnp.where(x == cx - 1, layers * cx + lay, c1 + 1)
        c1, c2 = strip(c1.astype(F32)), strip(c2.astype(F32))
        y1, y2 = strip(y), strip(y + 1.0)
        near, far = parts_of(val * (1.0 - fx)), parts_of(val * fx)
        low, high = parts_of(1.0 - fy), parts_of(fy)
        lh, ll = [pick_two(r_id, c1, c2, near[i], far[i]) for i in range(2)]
        rh, rl = [pick_two(y_id, y1, y2, low[i], high[i]) for i in range(2)]
        both = dot_nt(jnp.concatenate([rh, rl], axis=0), lh)
        acc[0:y_rows, 0:r_rows] += both[:y_rows] + both[y_rows:] + dot_nt(rh, ll)

    acc[...] = jnp.zeros_like(acc)

    @pl.when(jnp.logical_not(has_west))
    def _():
        east_in[...] = jnp.zeros_like(east_in)
        west_h[...] = jnp.zeros_like(west_h)

    @pl.when(jnp.logical_not(has_east))
    def _():
        east_h[...] = jnp.zeros_like(east_h)

    @pl.when(jnp.logical_not(has_south))
    def _():
        north_in[...] = jnp.zeros_like(north_in)

    @pl.when(jnp.logical_not(has_south & has_west))
    def _():
        corner_in[...] = jnp.zeros_like(corner_in)

    spread(packed[me])

    def receive(k, c):
        src = lax.rem(me + tiles - k, tiles)
        pltpu.make_async_remote_copy(
            src_ref=packed.at[src], dst_ref=recv.at[src], send_sem=s_send.at[src], recv_sem=s_recv.at[src],
            device_id=partner, device_id_type=MESH).wait_recv()
        spread(recv[src])
        return c

    lax.fori_loop(1, tiles, receive, 0)

    swap = pltpu.make_async_remote_copy(
        src_ref=acc.at[pl.ds(0, y_rows)], dst_ref=acc_in, send_sem=p_sem.at[0], recv_sem=p_sem.at[1],
        device_id=partner, device_id_type=MESH)
    swap.start()

    def remote(src, dst, send_sem, recv_sem, dev):
        return pltpu.make_async_remote_copy(src_ref=src, dst_ref=dst, send_sem=send_sem, recv_sem=recv_sem,
                                            device_id=dev, device_id_type=MESH)

    def start(copies):
        for c, sends, _ in copies:
            pl.when(sends)(c.start)

    def finish(copies):
        for c, sends, gets in copies:
            pl.when(gets)(c.wait_recv)
            pl.when(sends)(c.wait_send)

    e_tx, w_tx = lax.rem(tx + 1, n_tx), lax.rem(tx + n_tx - 1, n_tx)
    n_ty_id, s_ty_id = lax.rem(ty + 1, n_ty), lax.rem(ty + n_ty - 1, n_ty)
    rim_rows = pl.ds(layers * cx, 16)
    rims = []
    for q in range(n_mem):
        other = lax.rem(mem + q, n_mem)
        rims.append((remote(acc.at[pl.ds(cy, 8)], north_in.at[q], rim_send.at[0, q], rim_recv.at[0, q],
                            (tx, n_ty_id, other)), has_north, has_south))
    start(rims)
    gt[...] = acc[...].T
    late = []
    for q in range(n_mem):
        other = lax.rem(mem + q, n_mem)
        late.append((remote(gt.at[rim_rows, pl.ds(0, cy)], east_in.at[q], rim_send.at[1, q], rim_recv.at[1, q],
                            (e_tx, ty, other)), has_east, has_west))
        late.append((remote(gt.at[rim_rows, pl.ds(cy, cy)], corner_in.at[q], rim_send.at[2, q], rim_recv.at[2, q],
                            (e_tx, n_ty_id, other)), has_east & has_north, has_west & has_south))
    start(late)

    def drain(k, c):
        copy_to(lax.rem(me + k, tiles)).wait_send()
        return c

    lax.fori_loop(1, tiles, drain, 0)
    swap.wait()
    joined = jnp.concatenate([acc_in[...], jnp.zeros((2 * cy - y_rows, acc_in.shape[1]), F32)], axis=0).T
    grad = gt[0 : layers * cx, 0:cy] + joined[0 : layers * cx, 0:cy]
    finish(rims + late)
    north = sum(north_in[q] for q in range(n_mem))
    north = jnp.concatenate([north, jnp.zeros((cy - 8, north.shape[1]), F32)], axis=0)
    grad = grad + north.T[0 : layers * cx]
    east = sum(east_in[q] + corner_in[q] for q in range(n_mem))
    x_id = lax.broadcasted_iota(jnp.int32, (cx, cy), 0)
    g = [
        grad[k * cx : (k + 1) * cx] + jnp.where(x_id == 0, east[k : k + 1], 0.0)
        for k in range(layers)
    ]
    load.wait()

    def contract(m, c):
        for l in range(levels):
            total = jnp.zeros((cx, cy), F32)
            for t in range(slots):
                total = total + ens_v[m, t, l].astype(F32) * g[t * levels + l]
            con[m * levels + l] = total
            send_w[pl.ds(m * levels + l, 1), :] = total[0:1]
            send_e[pl.ds(m * levels + l, 1), :] = total[cx - 1 : cx]
        return c

    lax.fori_loop(0, members, contract, 0, unroll=2)

    def halo(i, src, dst, dev, sends, gets):
        return (remote(src, dst, halo_send.at[i], halo_recv.at[i], dev), sends, gets)

    sides = [halo(0, send_w, east_h, (w_tx, ty, mem), has_west, has_east),
             halo(1, send_e, west_h, (e_tx, ty, mem), has_east, has_west)]
    start(sides)
    planes = members * levels
    e_row = lax.broadcasted_iota(jnp.int32, (8, cy), 0)
    e_lane = lax.broadcasted_iota(jnp.int32, (8, cy), 1)
    pick = jnp.where((e_row == 0) & (e_lane == 0) | (e_row == 1) & (e_lane == cy - 1), 1.0, 0.0)
    exact = lax.Precision.HIGHEST
    corner_w[...] = dot_nt(pick, send_w[...], exact)
    corner_e[...] = dot_nt(pick, send_e[...], exact)
    edge[...] = dot_nt(pick, con[...].reshape(planes * cx, cy), exact)
    south = jnp.where((e_row == 1) & (e_lane == 0) & has_south, 0.25, 0.0)
    north = jnp.where((e_row == 0) & (e_lane == cy - 1) & has_north, 0.25, 0.0)
    always = tx >= 0
    places = [south + north] if n_ty == 2 else [south, north]
    targets = [n_ty_id, s_ty_id][: len(places)]
    for i, t in enumerate(targets):
        sides += [
            halo(2 + 3 * i, edge, edge_in.at[i], (tx, t, mem), always, always),
            halo(3 + 3 * i, corner_w, corner_from_e.at[i], (w_tx, t, mem), has_west, has_east),
            halo(4 + 3 * i, corner_e, corner_from_w.at[i], (e_tx, t, mem), has_east, has_west),
        ]
        pl.when(jnp.logical_not(has_east))(functools.partial(fill, corner_from_e, i))
        pl.when(jnp.logical_not(has_west))(functools.partial(fill, corner_from_w, i))
    start(sides[2:])

    batch = max(b for b in range(1, 11) if planes % b == 0)
    lane = lax.broadcasted_iota(jnp.int32, (batch * cx, cy), 1)
    x_in = lax.broadcasted_iota(jnp.int32, (batch * cx, cy), 0) % cx

    def local(i, c):
        here = pl.ds(i * batch, batch)
        mid = shift_mix(con[here].reshape(batch * cx, cy), 1, lane)
        before = jnp.where(x_in == 0, 0.0, pltpu.roll(mid, 1, 0))
        after = jnp.where(x_in == cx - 1, 0.0, pltpu.roll(mid, batch * cx - 1, 0))
        con[here] = (0.25 * before + 0.5 * mid + 0.25 * after).reshape(batch, cx, cy)
        return c

    lax.fori_loop(0, planes // batch, local, 0)
    finish(sides)

    def outer(e, place):
        return lax.dot_general(e, place, (((0,), (0,)), ((), ())), precision=exact, preferred_element_type=F32)

    l_in = lax.broadcasted_iota(jnp.int32, (8, planes * cx), 1) % cx
    row_lane = lax.broadcasted_iota(jnp.int32, (planes, cy), 1)
    west = shift_mix(west_h[...], 1, row_lane)
    east = shift_mix(east_h[...], 1, row_lane)
    added = jnp.zeros((planes * cx, cy), F32)
    for i, place in enumerate(places):
        e = edge_in[i]
        before = jnp.where(l_in == 0, 0.0, pltpu.roll(e, 1, 1))
        after = jnp.where(l_in == cx - 1, 0.0, pltpu.roll(e, planes * cx - 1, 1))
        added = added + outer(0.25 * before + 0.5 * e + 0.25 * after, place)
        west = west + outer(corner_from_w[i], place)
        east = east + outer(corner_from_e[i], place)
    fix[...] = added.reshape(planes, cx, cy)
    west_h[...] = 0.25 * west
    east_h[...] = 0.25 * east

    def last(m, c):
        for l in range(levels):
            i = m * levels + l
            res = con[i] + fix[i]
            res = res + jnp.where(x_id == 0, west_h[pl.ds(i, 1), :], 0.0)
            res = res + jnp.where(x_id == cx - 1, east_h[pl.ds(i, 1), :], 0.0)
            out[m, l] = res.astype(BF16)
        return c

    lax.fori_loop(0, members, last, 0, unroll=2)


def fill(ref, i):
    ref[i] = jnp.zeros(ref.shape[1:], F32)


def body(mesh_sizes, obs_value, obs_frac, obs_cell, obs_layer, obs_tile, obs_length, ensemble):
    n_tx, n_ty, n_mem = mesh_sizes
    tiles = n_tx * n_ty
    count = obs_value.shape[0]
    hi = pl.cdiv(3 * count // tiles, LO)
    members, slots, levels, cx, cy = ensemble.shape
    layers = slots * levels
    vmem = pl.BlockSpec(memory_space=pltpu.VMEM)
    smem = pl.BlockSpec(memory_space=pltpu.SMEM)
    rows = count // 128
    packed = pl.pallas_call(
        functools.partial(pack_kernel, tiles, hi, cx * cy),
        out_shape=jax.ShapeDtypeStruct((tiles, 4 * hi, LO), F32),
        in_specs=[vmem] * 5 + [smem],
        out_specs=vmem,
        scratch_shapes=[
            pltpu.VMEM((4 * tiles * hi, LO), F32),
            pltpu.VMEM((rows, 128), jnp.int32),
            pltpu.VMEM((rows, 128), jnp.int32),
            pltpu.VMEM((rows, 128), F32),
            pltpu.VMEM((rows, 128), jnp.int32),
        ],
    )(obs_value.reshape(rows, 128), obs_frac, obs_cell.reshape(rows, 128), obs_layer.reshape(rows, 128),
      obs_tile.reshape(rows, 128), obs_length)

    planes = members * levels
    y_rows = up_to(cy + 1, 16)
    square = 2 * cy
    sides = 1 if n_ty == 2 else 2
    dma = pltpu.SemaphoreType.DMA
    scratch = [
        pltpu.VMEM((tiles, 4 * hi, LO), F32),
        pltpu.VMEM((square, square), F32),
        pltpu.VMEM((y_rows, square), F32),
        pltpu.VMEM((square, square), F32),
        pltpu.VMEM((n_mem, 16, cy), F32),
        pltpu.VMEM((n_mem, 8, square), F32),
        pltpu.VMEM((n_mem, 16, cy), F32),
        pltpu.VMEM((planes, cx, cy), F32),
        pltpu.VMEM((planes, cx, cy), F32),
        pltpu.VMEM((planes, cy), F32),
        pltpu.VMEM((planes, cy), F32),
        pltpu.VMEM((planes, cy), F32),
        pltpu.VMEM((planes, cy), F32),
        pltpu.VMEM((8, planes * cx), F32),
        pltpu.VMEM((sides, 8, planes * cx), F32),
        pltpu.VMEM((8, planes), F32),
        pltpu.VMEM((8, planes), F32),
        pltpu.VMEM((sides, 8, planes), F32),
        pltpu.VMEM((sides, 8, planes), F32),
        pltpu.VMEM(ensemble.shape, BF16),
        dma((tiles,)), dma((tiles,)), dma((2,)), dma((3, n_mem)), dma((3, n_mem)),
        dma((2 + 3 * sides,)), dma((2 + 3 * sides,)), dma,
    ]
    dims = (n_tx, n_ty, n_mem, hi, layers, cx, cy, members, slots, levels)
    return pl.pallas_call(
        functools.partial(main_kernel, dims),
        out_shape=jax.ShapeDtypeStruct((members, levels, cx, cy), BF16),
        in_specs=[vmem, pl.BlockSpec(memory_space=pl.ANY)],
        out_specs=vmem,
        scratch_shapes=scratch,
        compiler_params=pltpu.CompilerParams(collective_id=0, has_side_effects=True),
    )(packed, ensemble)


def solution(mesh):
    placed = (
        P(("tx", "ty", "mem")),
        P(None, ("tx", "ty", "mem")),
        P(("tx", "ty", "mem")),
        P(("tx", "ty", "mem")),
        P(("tx", "ty", "mem")),
        P(("tx", "ty", "mem")),
        P("mem", None, None, "tx", "ty"),
    )
    sizes = tuple(mesh.shape[a] for a in ("tx", "ty", "mem"))
    return jax.shard_map(
        functools.partial(body, sizes), mesh=mesh, in_specs=placed, out_specs=P("mem", None, "tx", "ty"),
        check_vma=False,
    )
```
